256 devices in a mesh: cfg: 2 (over y), ta: 16 (over z), sa: 4 (over x), src: 2 (over core).
Axes of the slice: x: 4, y: 2, z: 16, core: 2. Of those that a mesh axis runs over, the one named last changes fastest.
The devices are a block of a 4x16x16 slice.
Arguments:
- prop: bfloat16 [4, 32, 2, 12, 12, 1024], P(('cfg', 'src'), 'ta', None, None, None, 'sa'), parts along dimension 0, may hold values from -6 to 6
- eps_rows: int32 [24, 3], replicated, may hold values from 0 to 11
- eps_sign: int32 [24], replicated, may hold values from 0 to 1
- source_sites: int32 [4, 3], P('cfg'), parts along dimension 0, may hold values from 0 to 15, as said below
- momenta: int32 [32, 3], replicated, may hold values from -2 to 2
Outputs:
- blocks: float32 [4, 32, 2, 32, 1728], P('cfg', None, None, 'ta', 'sa'), parts along dimension 0
The draws below stay inside these ranges and needn't reach their ends.
There are 2 independent parts, one for each index of `cfg`. The reference program is written for one: setup_inputs(seed, part) draws one part's arguments, and reference() takes and returns one part's arrays. A program takes and returns all parts, laid end to end along the dimension named above; an argument that names none is the same for every part. Nothing has to cross between parts.
Inputs may be any that keep to these rules, and one draw needn't show every extreme that they name: `source_sites`: each row is a lattice site: first coordinate below 4, second below 16, third below 16.
All inputs are finite; a program needn't handle non-finite values.
Results may differ from the reference program's by a relative error of at most 0.0045.
Values sent between devices are 32-bit elements; how exact they have to be, the bound alone decides.
A program may use at most 128 MiB of HBM per device.

```python
import math
import jax
import jax.numpy as jnp
from jax import lax

SC = 12
TERMS = 24
LY = 16
LZ = 16
BLOCK = 1728
LX = 4
SITES = 1024
TIMES = 32
NSRC = 2
MOM = 32


def draw_source_sites(key, part):
    key_x = jax.random.fold_in(key, 11)
    key_y = jax.random.fold_in(key, 12)
    key_z = jax.random.fold_in(key, 13)
    key_pick = jax.random.fold_in(key, 14)
    first = jax.random.randint(key_x, (NSRC,), 0, LX)
    second = jax.random.randint(key_y, (NSRC,), 0, LY)
    third = jax.random.randint(key_z, (NSRC,), 0, LZ)
    chosen = jax.random.randint(key_pick, (), 0, NSRC)
    follower = (chosen + 1) % NSRC
    rows = jnp.arange(NSRC, dtype=jnp.int32)
    corner = rows == chosen
    first = jnp.where(corner, LX - 1, first)
    second = jnp.where(corner, LY - 1, second)
    third = jnp.where(corner, LZ - 1, third)
    third = jnp.where(rows == follower, 0, third)
    return jnp.stack([first, second, third], axis=1).astype(jnp.int32)


def set_ends(entries, stream_key, least, top_value):
    longest = entries.shape.index(max(entries.shape))
    spots = []
    for shift in (0, 1):
        where = [jax.random.randint(jax.random.fold_in(stream_key, axis), (), 0, length) for axis, length in enumerate(entries.shape)]
        where[longest] = (where[longest] + shift) % entries.shape[longest]
        spots.append(tuple(where))
    return entries.at[spots[0]].set(least).at[spots[1]].set(top_value)


def shard_levels(stream_key, dims, shards, least, top_value):
    def one(axis_at, shards_of):
        steps = jax.random.uniform(jax.random.fold_in(jax.random.fold_in(stream_key, 6), axis_at), (shards_of,), jnp.float32, least / len(shards), top_value / len(shards))
        return jnp.repeat(jnp.exp(steps), dims[axis_at] // shards_of).reshape((-1,) + (1,) * (len(dims) - axis_at - 1))

    loudness = one(*shards[0])
    for cut in shards[1:]:
        loudness = loudness * one(*cut)
    return loudness


def normal_values(stream_key, dims, deviation, limit, pieces=(), kind=jnp.bfloat16):
    array = jax.random.normal(stream_key, dims, jnp.float32) * deviation
    if len(pieces) > 0:
        array = shard_levels(stream_key, dims, pieces, -0.22, 0.18) * array
    return jnp.clip(array, min=-limit, max=limit).astype(kind)


def setup_inputs(seed: int = 0, part: int = 0) -> dict:
    keys = jax.random.split(jax.random.key(seed), 6)
    part_splits = jax.random.split(jax.random.fold_in(keys[5], part), 6)
    return {
        "prop": normal_values(part_splits[0], (NSRC, TIMES, 2, SC, SC, SITES), 1.0, 6.0, ((0, 2), (1, 16), (5, 4))),
        "eps_rows": set_ends(jax.random.randint(keys[1], (TERMS, 3), 0, SC), jax.random.fold_in(keys[1], 1), 0, SC - 1).astype(jnp.int32),
        "eps_sign": set_ends(jax.random.randint(keys[2], (TERMS,), 0, 2), jax.random.fold_in(keys[2], 1), 0, 1).astype(jnp.int32),
        "source_sites": draw_source_sites(jax.random.fold_in(jax.random.fold_in(keys[5], part), 71), part),
        "momenta": set_ends(jax.random.randint(keys[4], (MOM, 3), -2, 3), jax.random.fold_in(keys[4], 1), -2, 2).astype(jnp.int32),
    }


def phase_table(position, momenta, site_index, extent_x):
    coord_x = site_index // (LY * LZ)
    coord_y = site_index // LZ % LY
    coord_z = site_index % LZ
    part_x = momenta[:, 0:1] * (coord_x[None, :] - position[0]) % extent_x
    part_y = momenta[:, 1:2] * (coord_y[None, :] - position[1]) % LY
    part_z = momenta[:, 2:3] * (coord_z[None, :] - position[2]) % LZ
    angle = 2.0 * math.pi * (part_x.astype(jnp.float32) / extent_x + part_y.astype(jnp.float32) / LY + part_z.astype(jnp.float32) / LZ)
    return jnp.concatenate([jnp.cos(angle), jnp.sin(angle)], axis=0).astype(jnp.bfloat16)

def contract(slab, rows, weights):
    first = jnp.take(slab, rows[:, 0], axis=1).astype(jnp.float32)
    second = jnp.take(slab, rows[:, 1], axis=1).astype(jnp.float32)
    third = jnp.take(slab, rows[:, 2], axis=1)
    scaled = weights[:, None, None, None]
    real = scaled * (first[0][:, :, None] * second[0][:, None] - first[1][:, :, None] * second[1][:, None])
    imag = scaled * (first[0][:, :, None] * second[1][:, None] + first[1][:, :, None] * second[0][:, None])
    pair = jnp.stack([real, imag]).astype(jnp.bfloat16)
    mixer = jnp.stack([jnp.stack([third[0], -third[1]]), jnp.stack([third[1], third[0]])])
    block = jnp.einsum('ceijx,oceLx->oijLx', pair.astype(jnp.float32), mixer.astype(jnp.float32))
    width = slab.shape[1]
    return block.astype(jnp.bfloat16).reshape(2 * width * width * width, slab.shape[-1])

def mix_phase(table, quark):
    product = jnp.dot(table, quark.T, preferred_element_type=jnp.float32)
    half_m = table.shape[0] // 2
    half_k = quark.shape[0] // 2
    cos_re = product[:half_m, :half_k]
    cos_im = product[:half_m, half_k:]
    sin_re = product[half_m:, :half_k]
    sin_im = product[half_m:, half_k:]
    return jnp.stack([cos_re + sin_im, cos_im - sin_re])

def reference(prop, eps_rows, eps_sign, source_sites, momenta):
    weights = (2 * eps_sign - 1).astype(jnp.float32)
    scale = 1.0 / math.sqrt(4.0 * TERMS * SITES)
    site_index = jnp.arange(SITES, dtype=jnp.int32)
    tables = jnp.stack([phase_table(source_sites[s], momenta, site_index, LX) for s in range(NSRC)])
    slabs = prop.reshape((NSRC * TIMES,) + prop.shape[2:])
    owners = jnp.repeat(jnp.arange(NSRC, dtype=jnp.int32), TIMES)

    def project(items):
        slab, owner = items
        quark = contract(slab, eps_rows, weights)
        return scale * mix_phase(tables[owner], quark)
    result = lax.map(project, (slabs, owners))
    return result.reshape(NSRC, TIMES, 2, MOM, BLOCK)
```

```python
import functools
import math

import jax
import jax.numpy as jnp
from jax import lax
from jax.experimental import pallas as pl
from jax.experimental.pallas import tpu as pltpu
from jax.sharding import PartitionSpec as P

LY = 16
LZ = 16
F32 = jnp.float32
BF16 = jnp.bfloat16
NT = (((1,), (1,)), ((), ()))


def split_rows(width, copies):
    rows = 2 * copies * width
    out = lax.broadcasted_iota(jnp.int32, (rows, 2 * width), 0)
    col = lax.broadcasted_iota(jnp.int32, (rows, 2 * width), 1)
    half = out // (copies * width)
    return (col == 2 * (out % width) + half).astype(F32).astype(BF16)


def group_kernel(terms, rows_ref, sign_ref, prop_ref, h_ref, f_ref, acc_ref):
    width = prop_ref.shape[1]
    sites = prop_ref.shape[3]
    spread = split_rows(width, 2)
    for r in range(width):
        both = jnp.dot(spread, prop_ref[0, r], preferred_element_type=F32)
        f_ref[r, 0] = both[: 2 * width]
        f_ref[r, 1] = both[2 * width :]
    acc_ref[...] = jnp.zeros_like(acc_ref)
    low = lax.broadcasted_iota(jnp.int32, (8, sites), 0) < 4

    def term(e, carry):
        r0, r1, r2 = rows_ref[0, e], rows_ref[1, e], rows_ref[2, e]
        w = (2 * sign_ref[0, e] - 1).astype(F32)
        re2 = [f_ref[r2, 0, 8 * k : 8 * k + 8, :] for k in range(3)]
        im2 = [f_ref[r2, 1, 8 * k : 8 * k + 8, :] for k in range(3)]
        for m in range(width // 2):
            re1 = [jnp.broadcast_to(f_ref[r1, 0, 2 * m + k : 2 * m + k + 1, :] * w, (8, sites)) for k in range(2)]
            im1 = [jnp.broadcast_to(f_ref[r1, 1, 2 * m + k : 2 * m + k + 1, :] * w, (8, sites)) for k in range(2)]
            re1 = [re1[0], jnp.where(low, re1[0], re1[1]), re1[1]]
            im1 = [im1[0], jnp.where(low, im1[0], im1[1]), im1[1]]
            for k in range(3):
                at = slice(24 * m + 8 * k, 24 * m + 8 * k + 8)
                acc_ref[r0, 0, at, :] += re1[k] * re2[k] - im1[k] * im2[k]
                acc_ref[r0, 1, at, :] += re1[k] * im2[k] + im1[k] * re2[k]
        return carry

    lax.fori_loop(0, terms, term, 0)
    for r in range(width):
        for c in range(2):
            h_ref[0, c, :, r * sites : (r + 1) * sites] = acc_ref[r, c].astype(BF16)


def cos16(k):
    k = k & 15
    k = jnp.minimum(k, 16 - k)
    out = jnp.full(k.shape, -1.0, F32)
    for n in range(8):
        out = jnp.where(k == n, F32(math.cos(math.pi * n / 8) if n != 4 else 0.0), out)
    return out.astype(BF16).astype(F32)


def column(row):
    n = row.shape[1]
    eye = lax.broadcasted_iota(jnp.int32, (n, n), 0) == lax.broadcasted_iota(jnp.int32, (n, n), 1)
    return jnp.sum(jnp.where(eye, jnp.broadcast_to(row.astype(F32), (n, n)), 0.0), axis=1, keepdims=True)


def phases(extent_x, mom_ref, site_ref, sites):
    mom = mom_ref.shape[1]
    src, sa = lax.axis_index("src"), lax.axis_index("sa")
    x = lax.broadcasted_iota(jnp.int32, (mom, sites), 1) + sa * sites
    where = (x // (LY * LZ), (x // LZ) % LY, x % LZ)
    total = jnp.zeros((mom, sites), jnp.int32)
    for d, extent in enumerate((extent_x, LY, LZ)):
        n = jnp.broadcast_to(column(mom_ref[d : d + 1, :]), (mom, sites)).astype(jnp.int32)
        total += (n * (where[d] - site_ref[src, d])) * (16 // extent)
    return cos16(total), cos16(total - 4)


def project(t, scale, prop_ref, h_ref, cos_ref, sin_ref, pf_ref, z_ref, v_ref, x_ref):
    width, sites = prop_ref.shape[1], prop_ref.shape[3]
    mom = cos_ref.shape[0]
    nsa, nta = x_ref.shape[1], x_ref.shape[2]
    third = width // nsa
    block = width * width
    spread = split_rows(width, 1)
    half = width * mom

    def one_row(r, carry):
        both = jnp.dot(spread, prop_ref[t, r], preferred_element_type=F32)
        at = pl.ds(pl.multiple_of(r * sites, sites), sites)
        cos, sin = cos_ref[...], sin_ref[...]
        for i in range(width):
            re, im = both[i : i + 1, :], both[width + i : width + i + 1, :]
            row = (i % third) * nsa * mom + (i // third) * mom
            pf_ref[row : row + mom, at] = (cos * re + sin * im).astype(BF16)
            pf_ref[half + row : half + row + mom, at] = (cos * im - sin * re).astype(BF16)
        return carry

    lax.fori_loop(0, width, one_row, 0)
    for c in range(2):
        z_ref[c] = lax.dot_general(pf_ref[...], h_ref[t, c], NT, preferred_element_type=F32)
    part = nsa * mom
    for c in range(2):
        for i in range(third):
            a, b = slice(i * part, (i + 1) * part), slice(half + i * part, half + (i + 1) * part)
            if c == 0:
                value = (z_ref[0, a, :] - z_ref[1, b, :]) * scale
            else:
                value = (z_ref[1, a, :] + z_ref[0, b, :]) * scale
            v_ref[:, i * block : (i + 1) * block] = value
        for s in range(nsa):
            x_ref[t, s, :, c] = v_ref[s * mom : (s + 1) * mom, :].reshape(nta, mom // nta, third * block)


def exchange_kernel(extent_x, scale, site_ref, mom_ref, prop_ref, h_ref, out_ref, *scratch):
    (cos_ref, sin_ref, pf_ref, z_ref, v_ref, x_ref, got1, got2, keep, relay, red) = scratch[:11]
    (s1_send, s1_recv, s2_send, s2_recv, a_send, a_recv, f_send, f_recv) = scratch[11:]
    times, nsa, nta = x_ref.shape[0], x_ref.shape[1], x_ref.shape[2]
    ta, sa, src = lax.axis_index("ta"), lax.axis_index("sa"), lax.axis_index("src")
    flip = sa + 1 - 2 * (sa % 2)
    mirror = nsa - 1 - sa
    mates = (flip, mirror)
    other = 1 - src
    hop = nta // 2

    barrier = pltpu.get_barrier_semaphore()
    for mate in mates:
        pl.semaphore_signal(barrier, inc=1, device_id={"sa": mate})
    pl.semaphore_signal(barrier, inc=1, device_id={"src": other})

    def greet(k, carry):
        pl.semaphore_signal(barrier, inc=1, device_id={"ta": (ta + k) % nta})
        return carry

    lax.fori_loop(1, nta, greet, 0)

    cos, sin = phases(extent_x, mom_ref, site_ref, prop_ref.shape[3])
    cos_ref[...] = cos
    sin_ref[...] = sin

    def first(t, half, slot):
        mate = mates[half]
        dest = mate if slot == 0 else nsa - 1 - mate if half == 0 else mate + 1 - 2 * (mate % 2)
        return pltpu.make_async_remote_copy(
            src_ref=x_ref.at[t, dest, pl.ds(half * hop, hop)],
            dst_ref=got1.at[t, half, slot],
            send_sem=s1_send.at[t, half, slot],
            recv_sem=s1_recv.at[t, half, slot],
            device_id={"sa": mate},
        )

    def second(t, half):
        return pltpu.make_async_remote_copy(
            src_ref=relay.at[t, half],
            dst_ref=got2.at[t, half],
            send_sem=s2_send.at[t, half],
            recv_sem=s2_recv.at[t, half],
            device_id={"sa": mates[1 - half]},
        )

    def spread(t, k):
        to = (ta + k) % nta
        return pltpu.make_async_remote_copy(
            src_ref=red.at[t, to],
            dst_ref=out_ref.at[src, ta, t],
            send_sem=a_send.at[t, k],
            recv_sem=a_recv.at[t, k],
            device_id={"ta": to},
        )

    def forward(t, k):
        at = (ta + nta - k) % nta
        return pltpu.make_async_remote_copy(
            src_ref=out_ref.at[src, at, t],
            dst_ref=out_ref.at[src, at, t],
            send_sem=f_send.at[t, k],
            recv_sem=f_recv.at[t, k],
            device_id={"src": other},
        )

    def start_first(t):
        for half in range(2):
            for slot in (1, 0):
                first(t, half, slot).start()

    def start_second(t):
        for half in range(2):
            first(t, half, 1).wait_recv()
            relay[t, half] = x_ref[t, mates[1 - half], half * hop : (half + 1) * hop] + got1[t, half, 1]
            second(t, half).start()
        for half in range(2):
            first(t, half, 0).wait_recv()
            keep[t, half] = x_ref[t, sa, half * hop : (half + 1) * hop] + got1[t, half, 0]

    def start_spread(t):
        for half in range(2):
            second(t, half).wait_recv()
            red[t, half * hop : (half + 1) * hop] = keep[t, half] + got2[t, half]
        for k in order(nta):
            spread(t, k).start()
        out_ref[src, ta, t] = red[t, ta]
        forward(t, 0).start()

    def collect(t):
        for k in reversed(order(nta)):
            spread(t, k).wait_recv()
            forward(t, k).start()

    for t in range(times):
        project(t, scale, prop_ref, h_ref, cos_ref, sin_ref, pf_ref, z_ref, v_ref, x_ref)
        if t == 0:
            pl.semaphore_wait(barrier, nta + 2)
        start_first(t)
        if t >= 1:
            start_second(t - 1)
            start_spread(t - 1)
    start_second(times - 1)
    for t in range(times - 1):
        collect(t)
    start_spread(times - 1)
    collect(times - 1)
    for t in range(times):
        for half in range(2):
            first(t, half, 0).wait_send()
            first(t, half, 1).wait_send()
            second(t, half).wait_send()
        for k in range(nta):
            if k > 0:
                spread(t, k).wait_send()
            forward(t, k).wait()


def order(nta):
    return sorted(range(1, nta), key=lambda k: (-min(k, nta - k), k))


def solution(mesh):
    nta, nsa = mesh.shape["ta"], mesh.shape["sa"]

    def per_device(prop, eps_rows, eps_sign, source_sites, momenta):
        times, width, sites = prop.shape[1], prop.shape[3], prop.shape[5]
        mom, terms = momenta.shape[0], eps_rows.shape[0]
        extent_x = sites * nsa // (LY * LZ)
        scale = 1.0 / math.sqrt(4.0 * terms * sites * nsa)
        block = width * width
        depth = width * sites
        slabs = prop.transpose(0, 1, 3, 4, 2, 5).reshape(times, width, 2 * width, sites)
        smem = pl.BlockSpec(memory_space=pltpu.SMEM)
        vmem = pl.BlockSpec(memory_space=pltpu.VMEM)
        h = pl.pallas_call(
            functools.partial(group_kernel, terms),
            grid=(times,),
            out_shape=jax.ShapeDtypeStruct((times, 2, block, depth), BF16),
            in_specs=[smem, smem, pl.BlockSpec((1, width, 2 * width, sites), lambda t: (t, 0, 0, 0))],
            out_specs=pl.BlockSpec((1, 2, block, depth), lambda t: (t, 0, 0, 0)),
            scratch_shapes=[
                pltpu.VMEM((width, 2, 2 * width, sites), F32),
                pltpu.VMEM((width, 2, block, sites), F32),
            ],
        )(eps_rows.T, eps_sign.reshape(1, terms), slabs)
        tail = (2, mom // nta, block * width // nsa)
        dma = pltpu.SemaphoreType.DMA
        out = pl.pallas_call(
            functools.partial(exchange_kernel, extent_x, scale),
            out_shape=jax.ShapeDtypeStruct((2, nta, times) + tail, F32),
            in_specs=[smem, vmem, vmem, vmem],
            out_specs=vmem,
            scratch_shapes=[
                pltpu.VMEM((mom, sites), F32),
                pltpu.VMEM((mom, sites), F32),
                pltpu.VMEM((2 * width * mom, depth), BF16),
                pltpu.VMEM((2, 2 * width * mom, block), F32),
                pltpu.VMEM((nsa * mom, block * width // nsa), F32),
                pltpu.VMEM((times, nsa, nta) + tail, F32),
                pltpu.VMEM((times, 2, 2, nta // 2) + tail, F32),
                pltpu.VMEM((times, 2, nta // 2) + tail, F32),
                pltpu.VMEM((times, 2, nta // 2) + tail, F32),
                pltpu.VMEM((times, 2, nta // 2) + tail, F32),
                pltpu.VMEM((times, nta) + tail, F32),
                dma((times, 2, 2)),
                dma((times, 2, 2)),
                dma((times, 2)),
                dma((times, 2)),
                dma((times, nta)),
                dma((times, nta)),
                dma((times, nta)),
                dma((times, nta)),
            ],
            compiler_params=pltpu.CompilerParams(collective_id=0, has_side_effects=True),
        )(source_sites, momenta.T, slabs, h)
        return out.reshape(2, nta * times, *tail)

    return jax.shard_map(
        per_device,
        mesh=mesh,
        in_specs=(P(("cfg", "src"), "ta", None, None, None, "sa"), P(), P(), P("cfg", None), P()),
        out_specs=P("cfg", None, None, "ta", "sa"),
        check_vma=False,
    )
```

```python
import functools
import math

import jax
import jax.numpy as jnp
from jax import lax
from jax.experimental import pallas as pl
from jax.experimental.pallas import tpu as pltpu
from jax.sharding import PartitionSpec as P

LY = 16
LZ = 16
F32 = jnp.float32
BF16 = jnp.bfloat16
PARTS = 4
NT = (((1,), (1,)), ((), ()))


def split_rows(width, copies):
    rows = 2 * copies * width
    out = lax.broadcasted_iota(jnp.int32, (rows, 2 * width), 0)
    col = lax.broadcasted_iota(jnp.int32, (rows, 2 * width), 1)
    half = out // (copies * width)
    return (col == 2 * (out % width) + half).astype(F32).astype(BF16)


def load_rows(prop_ref, f_ref):
    times, width, _, _, sites = prop_ref.shape
    spread = split_rows(width, 2)
    for t in range(times):
        for r in range(width):
            rows = prop_ref[t, r].reshape(2 * width, sites)
            both = jnp.dot(spread, rows, preferred_element_type=F32)
            f_ref[t, r, 0] = both[: 2 * width]
            f_ref[t, r, 1] = both[2 * width :]


def add_terms(t, terms, rows_ref, sign_ref, f_ref, sum_ref):
    width, sites = f_ref.shape[1], f_ref.shape[4]
    low = lax.broadcasted_iota(jnp.int32, (8, sites), 0) < 4
    sum_ref[0] = jnp.zeros(sum_ref.shape[1:], F32)
    batch = 2

    def term(e, last):
        r0, r1, r2 = rows_ref[0, e], rows_ref[1, e], rows_ref[2, e]
        w = (2 * sign_ref[0, e] - 1).astype(F32)
        before = jnp.int32(0)
        for r in range(width):
            before = jnp.where(r0 == r, last[r], before)
        re2 = [f_ref[t, r2, 0, 8 * k : 8 * k + 8, :] * w for k in range(3)]
        im2 = [f_ref[t, r2, 1, 8 * k : 8 * k + 8, :] * w for k in range(3)]
        for m0 in range(0, width // 2, batch):
            tiles = [(m, k) for m in range(m0, m0 + batch) for k in range(3)]
            old = [[sum_ref[before, c, 24 * m + 8 * k : 24 * m + 8 * k + 8, :] for c in range(2)] for m, k in tiles]
            for m in range(m0, m0 + batch):
                one = [
                    [jnp.broadcast_to(f_ref[t, r1, c, 2 * m + k : 2 * m + k + 1, :], (8, sites)) for k in range(2)]
                    for c in range(2)
                ]
                re1, im1 = [[rows[0], jnp.where(low, rows[0], rows[1]), rows[1]] for rows in one]
                for k in range(3):
                    at = slice(24 * m + 8 * k, 24 * m + 8 * k + 8)
                    old_re, old_im = old[tiles.index((m, k))]
                    sum_ref[e + 1, 0, at, :] = old_re + (re1[k] * re2[k] - im1[k] * im2[k])
                    sum_ref[e + 1, 1, at, :] = old_im + (re1[k] * im2[k] + im1[k] * re2[k])
        return tuple(jnp.where(r0 == r, e + 1, last[r]) for r in range(width))

    return lax.fori_loop(0, terms, term, (jnp.int32(0),) * width)


def cos16(k):
    k = k & 15
    k = jnp.minimum(k, 16 - k)
    out = jnp.full(k.shape, -1.0, F32)
    for n in range(8):
        out = jnp.where(k == n, F32(math.cos(math.pi * n / 8) if n != 4 else 0.0), out)
    return out.astype(BF16).astype(F32)


def step(n, nta):
    return nta // 2 + ((n + 1) // 2) * (1 - 2 * (n % 2))


def column(row):
    count = row.shape[1]
    nta = lax.axis_size("ta")
    near = count // nta
    at = lax.broadcasted_iota(jnp.int32, (count, count), 0)
    place = (lax.axis_index("ta") + step(at // near, nta)) % nta * near + at % near
    pick = lax.broadcasted_iota(jnp.int32, (count, count), 1) == place
    return jnp.sum(jnp.where(pick, jnp.broadcast_to(row.astype(F32), (count, count)), 0.0), axis=1, keepdims=True)


def phases(extent_x, mom_ref, site_ref, sites):
    mom = mom_ref.shape[1]
    src, sa = lax.axis_index("src"), lax.axis_index("sa")
    x = lax.broadcasted_iota(jnp.int32, (mom, sites), 1) + sa * sites
    where = (x // (LY * LZ), (x // LZ) % LY, x % LZ)
    total = jnp.zeros((mom, sites), jnp.int32)
    for d, extent in enumerate((extent_x, LY, LZ)):
        n = jnp.broadcast_to(column(mom_ref[d : d + 1, :]), (mom, sites)).astype(jnp.int32)
        total += (n * (where[d] - site_ref[src, d])) * (16 // extent)
    return cos16(total), cos16(total - 4)


def project(t, g, rows, last, sum_ref, f_ref, cos_ref, sin_ref, pf_ref, h_ref, z_ref):
    width, sites = f_ref.shape[1], f_ref.shape[4]
    mom = cos_ref.shape[0]
    nsa = lax.axis_size("sa")
    third = width // nsa
    half = width * mom
    slot = g % 2
    cos, sin = cos_ref[...], sin_ref[...]
    for n in range(rows):
        r = g * rows + n
        at = slice(n * sites, (n + 1) * sites)
        for c in range(2):
            h_ref[slot, c, :, at] = sum_ref[last[r], c].astype(BF16)
        for i in range(width):
            re, im = f_ref[t, r, 0, i : i + 1, :], f_ref[t, r, 1, i : i + 1, :]
            row = (i % third) * nsa * mom + (i // third) * mom
            pf_ref[slot, row : row + mom, at] = (cos * re + sin * im).astype(BF16)
            pf_ref[slot, half + row : half + row + mom, at] = (cos * im - sin * re).astype(BF16)
    for c in range(2):
        more = lax.dot_general(pf_ref[slot], h_ref[slot, c], NT, preferred_element_type=F32)
        z_ref[c] = more if g == 0 else z_ref[c] + more


def arrange(t, scale, z_ref, v_ref, x_ref):
    nsa, nta, _, near, run = x_ref.shape[1:]
    block = z_ref.shape[2]
    half = z_ref.shape[1] // 2
    part = nsa * nta * near
    for c in range(2):
        for i in range(run // block):
            a, b = slice(i * part, (i + 1) * part), slice(half + i * part, half + (i + 1) * part)
            if c == 0:
                value = (z_ref[0, a, :] - z_ref[1, b, :]) * scale
            else:
                value = (z_ref[1, a, :] + z_ref[0, b, :]) * scale
            v_ref[:, i * block : (i + 1) * block] = value
        for s in range(nsa):
            x_ref[t, s, :, c] = v_ref[s * nta * near : (s + 1) * nta * near, :].reshape(nta, near, run)


def blocks_kernel(extent_x, terms, scale, *refs):
    given, out_ref, held, load_sem, scratch = refs[:5], refs[5], refs[6:11], refs[11], refs[12:]
    site_ref, rows_ref, sign_ref, mom_ref, prop_ref = held
    (cos_ref, sin_ref, f_ref, sum_ref, pf_ref, h_ref, z_ref, v_ref) = scratch[:8]
    (x_ref, got1, got2, relay, red) = scratch[8:13]
    (s1_send, s1_recv, s2_send, s2_recv, a_send, a_recv, f_send, f_recv) = scratch[13:]
    times, nsa, nta = x_ref.shape[0], x_ref.shape[1], x_ref.shape[2]
    width = prop_ref.shape[1]
    parts, hop = got2.shape[1], got2.shape[3]
    ta, sa, src = lax.axis_index("ta"), lax.axis_index("sa"), lax.axis_index("src")
    flip = sa + 1 - 2 * (sa % 2)
    mirror = nsa - 1 - sa
    mates = (flip, mirror)
    other = 1 - src

    barrier = pltpu.get_barrier_semaphore()
    for n in range(nta - 1):
        pl.semaphore_signal(barrier, inc=1, device_id={"ta": (ta + step(n, nta)) % nta})
    for mate in mates:
        pl.semaphore_signal(barrier, inc=1, device_id={"sa": mate})
    pl.semaphore_signal(barrier, inc=1, device_id={"src": other})

    def span(q, half):
        return slice((2 * q + half) * hop, (2 * q + half + 1) * hop)

    def first(t, q, half, slot):
        mate = mates[half]
        dest = mate if slot == 0 else nsa - 1 - mate if half == 0 else mate + 1 - 2 * (mate % 2)
        return pltpu.make_async_remote_copy(
            src_ref=x_ref.at[t, dest, span(q, half)],
            dst_ref=got1.at[t, q, half, slot],
            send_sem=s1_send.at[t, q, half, slot],
            recv_sem=s1_recv.at[t, q, half, slot],
            device_id={"sa": mate},
        )

    def second(t, q, half):
        return pltpu.make_async_remote_copy(
            src_ref=relay.at[t, q, half],
            dst_ref=got2.at[t, q, half],
            send_sem=s2_send.at[t, q, half],
            recv_sem=s2_recv.at[t, q, half],
            device_id={"sa": mates[1 - half]},
        )

    def spread(t, n):
        return pltpu.make_async_remote_copy(
            src_ref=red.at[t, n],
            dst_ref=out_ref.at[src, ta, t],
            send_sem=a_send.at[t, n],
            recv_sem=a_recv.at[t, n],
            device_id={"ta": (ta + step(n, nta)) % nta},
        )

    def forward(t, n):
        at = (ta + nta - step(n, nta)) % nta
        return pltpu.make_async_remote_copy(
            src_ref=out_ref.at[src, at, t],
            dst_ref=out_ref.at[src, at, t],
            send_sem=f_send.at[t, n],
            recv_sem=f_recv.at[t, n],
            device_id={"src": other},
        )

    def start_first(t, q):
        for slot in (1, 0):
            for half in range(2):
                first(t, q, half, slot).start()

    def start_second(t, q):
        for half in range(2):
            first(t, q, half, 1).wait_recv()
            relay[t, q, half] = x_ref[t, mates[1 - half], span(q, half)] + got1[t, q, half, 1]
            second(t, q, half).start()

    def start_spread(t, q):
        for half in range(2):
            first(t, q, half, 0).wait_recv()
            second(t, q, half).wait_recv()
            red[t, span(q, half)] = x_ref[t, sa, span(q, half)] + got1[t, q, half, 0] + got2[t, q, half]
            for n in range((2 * q + half) * hop, (2 * q + half + 1) * hop):
                if n < nta - 1:
                    spread(t, n).start()
                else:
                    out_ref[src, ta, t] = red[t, n]
                    forward(t, n).start()

    def collect(t):
        for n in range(nta - 1):
            spread(t, n).wait_recv()
            forward(t, n).start()

    loads = [pltpu.make_async_copy(a, b, load_sem.at[n]) for n, (a, b) in enumerate(zip(given, held))]
    for load in loads:
        load.start()
    for load in loads[:4]:
        load.wait()
    cos, sin = phases(extent_x, mom_ref, site_ref, prop_ref.shape[4])
    cos_ref[...] = cos
    sin_ref[...] = sin
    loads[4].wait()
    load_rows(prop_ref, f_ref)
    groups = 3
    for t in range(times):
        last = add_terms(t, terms, rows_ref, sign_ref, f_ref, sum_ref)
        if t == 1:
            pl.semaphore_wait(barrier, nta + 2)
            for q in range(parts):
                start_first(t - 1, q)
        for g in range(groups):
            project(t, g, width // groups, last, sum_ref, f_ref, cos_ref, sin_ref, pf_ref, h_ref, z_ref)
            if t > 0 and g == 1:
                start_second(t - 1, 0)
        if t > 0:
            for q in range(1, parts):
                start_second(t - 1, q)
        arrange(t, scale, z_ref, v_ref, x_ref)
        if t > 0:
            for q in range(parts):
                start_first(t, q)
            for q in range(parts):
                start_spread(t - 1, q)
    t = times - 1
    for q in range(parts):
        start_second(t, q)
        if q > 0:
            start_spread(t, q - 1)
    start_spread(t, parts - 1)
    for t in range(times):
        collect(t)
    for t in range(times):
        for q in range(parts):
            for half in range(2):
                first(t, q, half, 0).wait_send()
                first(t, q, half, 1).wait_send()
                second(t, q, half).wait_send()
        for n in range(nta):
            if n < nta - 1:
                spread(t, n).wait_send()
            forward(t, n).wait()


def solution(mesh):
    nta, nsa = mesh.shape["ta"], mesh.shape["sa"]

    def per_device(prop, eps_rows, eps_sign, source_sites, momenta):
        times, width, sites = prop.shape[1], prop.shape[3], prop.shape[5]
        mom, terms = momenta.shape[0], eps_rows.shape[0]
        extent_x = sites * nsa // (LY * LZ)
        scale = 1.0 / math.sqrt(4.0 * terms * sites * nsa)
        block = width * width
        slabs = prop.transpose(0, 1, 3, 4, 2, 5).reshape(times, width, width, 2, sites)
        tail = (2, mom // nta, block * width // nsa)
        rows = width // 3
        parts = PARTS if nta % (2 * PARTS) == 0 else 1
        hop = nta // (2 * parts)
        dma = pltpu.SemaphoreType.DMA
        out = pl.pallas_call(
            functools.partial(blocks_kernel, extent_x, terms, scale),
            out_shape=jax.ShapeDtypeStruct((2, nta, times) + tail, F32),
            in_specs=[pl.BlockSpec(memory_space=pltpu.HBM)] * 5,
            out_specs=pl.BlockSpec(memory_space=pltpu.VMEM),
            scratch_shapes=[
                pltpu.SMEM(source_sites.shape, jnp.int32),
                pltpu.SMEM((3, terms), jnp.int32),
                pltpu.SMEM((1, terms), jnp.int32),
                pltpu.VMEM((3, mom), jnp.int32),
                pltpu.VMEM(slabs.shape, BF16),
                dma((5,)),
                pltpu.VMEM((mom, sites), F32),
                pltpu.VMEM((mom, sites), F32),
                pltpu.VMEM((times, width, 2, 2 * width, sites), F32),
                pltpu.VMEM((terms + 1, 2, block, sites), F32),
                pltpu.VMEM((2, 2 * width * mom, rows * sites), BF16),
                pltpu.VMEM((2, 2, block, rows * sites), BF16),
                pltpu.VMEM((2, 2 * width * mom, block), F32),
                pltpu.VMEM((nsa * mom, block * width // nsa), F32),
                pltpu.VMEM((times, nsa, nta) + tail, F32),
                pltpu.VMEM((times, parts, 2, 2, hop) + tail, F32),
                pltpu.VMEM((times, parts, 2, hop) + tail, F32),
                pltpu.VMEM((times, parts, 2, hop) + tail, F32),
                pltpu.VMEM((times, nta) + tail, F32),
                dma((times, parts, 2, 2)),
                dma((times, parts, 2, 2)),
                dma((times, parts, 2)),
                dma((times, parts, 2)),
                dma((times, nta)),
                dma((times, nta)),
                dma((times, nta)),
                dma((times, nta)),
            ],
            compiler_params=pltpu.CompilerParams(
                collective_id=0, has_side_effects=True, vmem_limit_bytes=32 * 1024 * 1024
            ),
        )(source_sites, eps_rows.T, eps_sign.reshape(1, terms), momenta.T, slabs)
        return out.reshape(2, nta * times, *tail)

    return jax.shard_map(
        per_device,
        mesh=mesh,
        in_specs=(P(("cfg", "src"), "ta", None, None, None, "sa"), P(), P(), P("cfg", None), P()),
        out_specs=P("cfg", None, None, "ta", "sa"),
        check_vma=False,
    )
```
